128 devices in a mesh: gz: 128 (over y, x, z, core).
Axes of the slice: x: 4, y: 4, z: 4, core: 2. Of those that a mesh axis runs over, the one named last changes fastest.
Arguments:
- u_face: float32 [256, 1024, 512], P('gz')
- v_face: float32 [256, 1024, 512], P('gz')
- w_face: float32 [256, 1024, 512], P('gz')
- smoke: float32 [256, 1024, 512], P('gz'), may hold values from 0 to 2
- obstacles: int32 [256, 32, 512], P('gz'), may hold values from -2147483648 to 2147483647, as said below
Outputs:
- impulse: float32 [256, 1024, 512], P('gz')
- relative_residual: float32 [256, 1024, 512], P('gz')
The draws below stay inside these ranges and needn't reach their ends.
Inputs may be any that keep to these rules, and one draw needn't show every extreme that they name: Bit k of obstacles[z, b, x] is 1 where cell (z, 32 b + k, x) is solid and 0 where it holds fluid; every bit of a word is used.
All inputs are finite; a program needn't handle non-finite values. Where the reference program divides by a largest or mean magnitude, that divisor is 1e-20 or more.
Results may differ from the reference program's by a relative error of at most 0.00011.
Values sent between devices are 32-bit elements; how exact they have to be, the bound alone decides.
A program may use at most 192 MiB of HBM per device.

```python
import jax
import jax.numpy as jnp
from jax import lax

NX = 512
NY = 1024
ITERS = 2
NZ = 256


def velocity_field(key):
    first = jax.random.fold_in(key, 0)
    depth = jnp.arange(NZ, dtype=jnp.float32) / max(NZ - 1, 1)
    ramp = 1.0 + 2.0 * depth[:, None, None]
    base = jax.random.normal(first, (NZ, NY, NX), jnp.float32)
    return jnp.clip(base, -6.0, 6.0) * ramp


def draw_u_face(key, part):
    return velocity_field(jax.random.fold_in(key, 11))


def draw_v_face(key, part):
    return velocity_field(jax.random.fold_in(key, 23))


def draw_w_face(key, part):
    return velocity_field(jax.random.fold_in(key, 37))


def draw_obstacles(key, part):
    first, second = jax.random.split(jax.random.fold_in(key, 53))
    shape = (NZ, NY // 32, NX)
    left = jax.random.randint(first, shape, -2147483648, 2147483647, dtype=jnp.int32)
    right = jax.random.randint(second, shape, -2147483648, 2147483647, dtype=jnp.int32)
    return left & right


def levels(stream_key, shape, cuts, smallest, largest):
    gain, own = 1.0, jax.random.fold_in(stream_key, 6)
    for position, blocks in cuts:
        steps = jnp.exp(jax.random.uniform(jax.random.fold_in(own, position), (blocks,), jnp.float32, smallest / len(cuts), largest / len(cuts)))
        gain = gain * jnp.repeat(steps, shape[position] // blocks).reshape([-1 if axis == position else 1 for axis in range(len(shape))])
    return gain


def setup_inputs(seed: int = 0) -> dict:
    splits = jax.random.split(jax.random.key(seed), 6)
    return {
        "u_face": draw_u_face(jax.random.fold_in(splits[5], 71), 0),
        "v_face": draw_v_face(jax.random.fold_in(splits[5], 71), 0),
        "w_face": draw_w_face(jax.random.fold_in(splits[5], 71), 0),
        "smoke": jnp.clip(2.0 * jax.random.uniform(splits[3], (NZ, NY, NX), jnp.float32) ** levels(splits[3], (NZ, NY, NX), ((0, 128),), -0.2, 0.2), 0.0, 2.0),
        "obstacles": draw_obstacles(jax.random.fold_in(splits[5], 71), 0),
    }


EPS = 1e-06
CFL = 0.5
BUOYANCY = 100.0

def unpack_flags(packed):
    places = jnp.arange(32, dtype=jnp.int32)
    flags = jnp.right_shift(packed[:, :, None, :], places[None, None, :, None]) & 1
    return flags.reshape(packed.shape[0], packed.shape[1] * 32, packed.shape[2])

def next_along(field, axis):
    widths = [(0, 0), (0, 0), (0, 0)]
    widths[axis] = (0, 1)
    padded = jnp.pad(field, widths)
    return lax.slice_in_dim(padded, 1, field.shape[axis] + 1, axis=axis)

def neighbour_sum(field):
    padded = jnp.pad(field, 1)
    total = padded[2:, 1:-1, 1:-1] + padded[:-2, 1:-1, 1:-1]
    total = total + padded[1:-1, 2:, 1:-1] + padded[1:-1, :-2, 1:-1]
    return total + padded[1:-1, 1:-1, 2:] + padded[1:-1, 1:-1, :-2]

def reference(u_face, v_face, w_face, smoke, obstacles):
    solid_cells = unpack_flags(obstacles).astype(jnp.float32)
    fluid_cells = 1.0 - solid_cells
    fastest = jnp.maximum(jnp.maximum(jnp.max(jnp.abs(u_face)), jnp.max(jnp.abs(v_face))), jnp.max(jnp.abs(w_face)))
    time_step = CFL / (fastest + EPS)
    lift = time_step * BUOYANCY
    lifted_w = w_face + lift * smoke
    divergence = fluid_cells * (next_along(u_face, 2) - u_face + (next_along(v_face, 1) - v_face) + (next_along(lifted_w, 0) - lifted_w))
    div_squares = jnp.sum(divergence * divergence)
    fluid_total = jnp.maximum(jnp.sum(fluid_cells), 1.0)
    open_count = 6.0 - neighbour_sum(solid_cells)
    scaling = fluid_cells * jnp.maximum(open_count, 1.0) + solid_cells

    def apply_operator(search):
        return fluid_cells * (open_count * search - neighbour_sum(fluid_cells * search)) + solid_cells * search
    residual = divergence / time_step
    solution = jnp.zeros_like(residual)
    search = residual / scaling
    rz_now = jnp.sum(residual * residual / scaling)
    for step in range(ITERS):
        image = apply_operator(search)
        alpha = rz_now / jnp.sum(search * image)
        solution = solution + alpha * search
        residual = residual - alpha * image
        if step + 1 < ITERS:
            precond = residual / scaling
            rz_next = jnp.sum(residual * precond)
            search = precond + rz_next / rz_now * search
            rz_now = rz_next
    impulse = time_step * solution
    relative_residual = residual * time_step / jnp.sqrt(div_squares / fluid_total + EPS)
    return (impulse, relative_residual)
```

```python
import functools

import jax
import jax.numpy as jnp
from jax import lax
from jax.experimental import pallas as pl
from jax.experimental.pallas import tpu as pltpu
from jax.sharding import PartitionSpec as P

EPS = 1e-06
CFL = 0.5
BUOYANCY = 100.0
MESH = pl.DeviceIdType.MESH

R = 32
CH = 64
LOAD = 256
PAD = 8
STAGES = ((1, 8, 0), (8, 4, 8), (32, 4, 12))
SLOTS = 16


def kernel(
    planes, rows, cols, devices,
    u_hbm, v_hbm, w_hbm, s_hbm, o_hbm, imp, rel,
    U, V, W, SM, FL, CNT, Z0, Z1, G, H, RED, ACC,
    load_sem, flag_sem, fs, fr, bs, br, lws, lwr, z0ds, z0dr, z1ds, z1dr, z0us, z0ur, z1us, z1ur,
    reds, redr,
):
    me = lax.axis_index("gz")
    low, high = me - 1, me + 1
    has_low, has_high = me > 0, me < devices - 1
    chunks = rows // CH
    early = chunks // 4
    loads = rows // LOAD
    lane = lax.broadcasted_iota(jnp.int32, (R, cols), 1)

    def peer(stride, n, k):
        pos = lax.rem(lax.div(me, stride), n)
        return me + (lax.rem(pos + k, n) - pos) * stride

    def load(a, p, q):
        src = (u_hbm, v_hbm, w_hbm, s_hbm)[a]
        dst = (U, V, W, SM)[a]
        span = pl.ds(q * LOAD, LOAD)
        return pltpu.make_async_copy(src.at[p, span], dst.at[p, span], load_sem.at[a, p, q])

    for p in range(planes):
        for q in range(loads):
            for a in range(3):
                load(a, p, q).start()
    flags_in = pltpu.make_async_copy(o_hbm, FL.at[pl.ds(1, planes)], flag_sem)
    flags_in.start()
    for p in range(planes):
        for q in range(loads):
            load(3, p, q).start()

    barrier = pltpu.get_barrier_semaphore()
    peers = 0
    for stride, n, _ in STAGES:
        for k in range(1, n):
            peers += 1
            pl.semaphore_signal(barrier, inc=1, device_id=(peer(stride, n, k),), device_id_type=MESH)

    @pl.when(has_low)
    def _():
        pl.semaphore_signal(barrier, inc=1, device_id=(low,), device_id_type=MESH)

    @pl.when(has_high)
    def _():
        pl.semaphore_signal(barrier, inc=1, device_id=(high,), device_id_type=MESH)

    V[:, pl.ds(rows, PAD), :] = jnp.zeros((planes, PAD, cols), jnp.float32)
    for Z in (Z0, Z1):
        for p in (1, 2):
            Z[p, pl.ds(0, PAD), :] = jnp.zeros((PAD, cols), jnp.float32)
            Z[p, pl.ds(PAD + rows, PAD), :] = jnp.zeros((PAD, cols), jnp.float32)

    def blocks(body, carry, first=0, last=rows // R):
        return lax.fori_loop(first, last, lambda b, c: body(pl.multiple_of(b * R, R), c), carry)

    def clear(refs):
        def body(r, c):
            for ref in refs:
                ref[pl.ds(r, R), :] = jnp.zeros((R, cols), jnp.float32)
            return c

        blocks(body, 0)

    @pl.when(jnp.logical_not(has_low))
    def _():
        FL[0] = jnp.zeros(FL.shape[1:], jnp.int32)
        for Z in (Z0, Z1):
            clear([Z.at[0, pl.ds(PAD, rows)]])

    @pl.when(jnp.logical_not(has_high))
    def _():
        FL[3] = jnp.zeros(FL.shape[1:], jnp.int32)
        clear([W.at[2], SM.at[2], Z0.at[3, pl.ds(PAD, rows)], Z1.at[3, pl.ds(PAD, rows)]])

    sides = jnp.where(has_low, 1, 0) + jnp.where(has_high, 1, 0)
    pl.semaphore_wait(barrier, peers + sides)

    def remote(src, dst, ss, rs, dev):
        return pltpu.make_async_remote_copy(
            src_ref=src, dst_ref=dst, send_sem=ss, recv_sem=rs, device_id=(dev,), device_id_type=MESH
        )

    def span(c, pad):
        return pl.ds(pl.multiple_of(c * CH + pad, 8), CH)

    def flags_copy(up):
        if up:
            return remote(o_hbm.at[planes - 1], FL.at[0], fs.at[0], fr.at[0], high)
        return remote(o_hbm.at[0], FL.at[3], fs.at[1], fr.at[1], low)

    def early_copy(a, c):
        src, dst = ((w_hbm, W), (s_hbm, SM))[a]
        return remote(src.at[0, span(c, 0)], dst.at[2, span(c, 0)], bs.at[a, c], br.at[a, c], low)

    def lw_copy(c):
        return remote(W.at[0, span(c, 0)], W.at[2, span(c, 0)], lws.at[c], lwr.at[c], low)

    def z_copy(Z, up, c):
        if up:
            ss, rs = (z0us, z0ur) if Z is Z0 else (z1us, z1ur)
            return remote(Z.at[2, span(c, PAD)], Z.at[0, span(c, PAD)], ss.at[c], rs.at[c], high)
        ss, rs = (z0ds, z0dr) if Z is Z0 else (z1ds, z1dr)
        return remote(Z.at[1, span(c, PAD)], Z.at[3, span(c, PAD)], ss.at[c], rs.at[c], low)

    def each(first, last, body):
        lax.fori_loop(first, last, lambda c, x: (body(c), x)[1], 0)

    @pl.when(has_low)
    def _():
        flags_copy(False).start()

        def body(c):
            early_copy(0, c).start()
            early_copy(1, c).start()

        each(0, early, body)

    @pl.when(has_high)
    def _():
        flags_copy(True).start()

    def red_copy(i, s, k, n_rows):
        stride, n, base = STAGES[s]
        part = pl.ds(0, n_rows)
        return remote(
            RED.at[i, base, part], RED.at[i, base + k, part], reds.at[i, base + k], redr.at[i, base + k],
            peer(stride, n, k),
        )

    def red_send(i, s, value):
        n_rows = value.shape[0]
        RED[i, STAGES[s][2], pl.ds(0, n_rows), :] = value
        for k in range(1, STAGES[s][1]):
            red_copy(i, s, k, n_rows).start()

    def red_wait(i, s, n_rows, op):
        _, n, base = STAGES[s]
        for k in range(1, n):
            red_copy(i, s, k, n_rows).wait_recv()
        total = RED[i, base, pl.ds(0, n_rows), :]
        for k in range(1, n):
            total = op(total, RED[i, base + k, pl.ds(0, n_rows), :])
        return total

    def red_end(i, n_rows):
        for s in range(3):
            for k in range(1, STAGES[s][1]):
                red_copy(i, s, k, n_rows).wait_send()

    def fold(x, op=jnp.add):
        return functools.reduce(op, [x[8 * i : 8 * i + 8] for i in range(x.shape[0] // 8)])

    def lanes(x, op=jnp.add):
        return functools.reduce(op, [x[:, 128 * i : 128 * i + 128] for i in range(x.shape[1] // 128)])

    def full(x):
        return jnp.full((8, 128), x, jnp.float32)

    top = jnp.zeros((8, cols), jnp.float32)
    for p in range(planes):
        for q in range(loads):
            for a in range(3):
                load(a, p, q).wait()

            def body(r, acc, p=p):
                m = jnp.maximum(
                    jnp.maximum(jnp.abs(U[p, pl.ds(r, R), :]), jnp.abs(V[p, pl.ds(r, R), :])),
                    jnp.abs(W[p, pl.ds(r, R), :]),
                )
                return jnp.maximum(acc, fold(m, jnp.maximum))

            top = blocks(body, top, q * LOAD // R, (q + 1) * LOAD // R)
    red_send(0, 0, lanes(top, jnp.maximum))

    flags_in.wait()

    @pl.when(has_low)
    def _():
        flags_copy(True).wait_recv()

    @pl.when(has_high)
    def _():
        flags_copy(False).wait_recv()

    words = rows // 32
    w_lane = lax.broadcasted_iota(jnp.int32, (words, cols), 1)
    w_row = lax.broadcasted_iota(jnp.int32, (words, cols), 0)
    for p in range(planes):
        c = FL[p + 1]
        zero = jnp.zeros_like(c)
        left = jnp.where(w_lane == 0, zero, pltpu.roll(c, 1, 1))
        right = jnp.where(w_lane == cols - 1, zero, pltpu.roll(c, cols - 1, 1))
        before = jnp.where(w_row == 0, zero, pltpu.roll(c, 1, 0))
        after = jnp.where(w_row == words - 1, zero, pltpu.roll(c, words - 1, 0))
        back = jnp.left_shift(c, 1) | lax.shift_right_logical(before, jnp.full_like(c, 31))
        ahead = lax.shift_right_logical(c, jnp.full_like(c, 1)) | jnp.left_shift(after, 31)
        below, above = FL[p], FL[p + 2]
        s1 = left ^ right ^ back
        c1 = (left & right) | (back & (left ^ right))
        s2 = ahead ^ below ^ above
        c2 = (ahead & below) | (above & (ahead ^ below))
        c3 = s1 & s2
        CNT[0, p] = s1 ^ s2
        CNT[1, p] = c1 ^ c2 ^ c3
        CNT[2, p] = (c1 & c2) | (c3 & (c1 ^ c2))
    for q in range(loads):
        for p in range(planes):
            load(3, p, q).wait()

    part = red_wait(0, 0, 8, jnp.maximum)
    red_send(0, 1, part)
    part = red_wait(0, 1, 8, jnp.maximum)
    red_send(0, 2, part)
    part = red_wait(0, 2, 8, jnp.maximum)
    step_v = CFL / (full(jnp.max(part)) + EPS)
    time_step = step_v[0, 0]
    lift = (step_v * BUOYANCY)[0, 0]
    per_step = (1.0 / step_v)[0, 0]

    def lift_block(p):
        def body(r, c):
            rs = pl.ds(r, R)
            W[p, rs, :] = W[p, rs, :] + lift * SM[p, rs, :]
            return c

        return body

    per = CH // R

    def lift_send(c):
        blocks(lift_block(0), 0, c * per, (c + 1) * per)

        @pl.when(has_low)
        def _():
            lw_copy(c).start()

    each(early, chunks, lift_send)
    blocks(lift_block(0), 0, 0, early * per)
    blocks(lift_block(1), 0)

    bit = lax.broadcasted_iota(jnp.int32, (R, cols), 0)

    def flag_block(p):
        def body(b, c):
            def bits(ref):
                return jnp.right_shift(jnp.broadcast_to(ref, (R, cols)), bit) & 1

            one = pl.ds(b, 1)
            solid = bits(FL[p + 1, one, :])
            count = (
                bits(CNT[0, p, one, :])
                + jnp.left_shift(bits(CNT[1, p, one, :]), 1)
                + jnp.left_shift(bits(CNT[2, p, one, :]), 2)
            )
            opened = (6 - count).astype(jnp.float32)
            wet = solid == 0
            rs = pl.ds(pl.multiple_of(b * R, R), R)
            H[p, rs, :] = jnp.where(wet, opened, 0.0)
            G[p, rs, :] = jnp.where(wet, 1.0 / jnp.maximum(opened, 1.0), 0.0)
            return c

        lax.fori_loop(0, rows // R, body, 0)

    def to_right(x):
        return jnp.where(lane == 0, 0.0, pltpu.roll(x, 1, 1))

    def to_left(x):
        return jnp.where(lane == cols - 1, 0.0, pltpu.roll(x, cols - 1, 1))

    def rhs_block(p):
        def body(r, acc):
            div_sum, wet_sum, gamma = acc
            rs = pl.ds(r, R)
            u, g = U[p, rs, :], G[p, rs, :]
            vb = V[p, pl.ds(r, R + PAD), :]
            v_next = pltpu.roll(vb, R + PAD - 1, 0)[:R]
            flat = (to_left(u) - u) + (v_next - vb[:R])
            wet = g > 0.0
            div = jnp.where(wet, flat + (W[p + 1, rs, :] - W[p, rs, :]), 0.0)
            r0 = div * per_step
            z0 = g * r0
            Z0[p + 1, pl.ds(pl.multiple_of(r + PAD, 8), R), :] = z0
            return (
                div_sum + fold(div * div),
                wet_sum + fold(jnp.where(wet, 1.0, 0.0)),
                gamma + fold(r0 * z0),
            )

        return body

    def chunk_loop(body, carry):
        return lax.fori_loop(0, chunks, body, carry)

    nil = jnp.zeros((8, cols), jnp.float32)
    flag_block(0)

    def first_rhs(c, acc):
        acc = blocks(rhs_block(0), acc, c * per, (c + 1) * per)

        @pl.when(has_low)
        def _():
            z_copy(Z0, False, c).start()

        return acc

    acc = chunk_loop(first_rhs, (nil, nil, nil))
    flag_block(1)

    @pl.when(has_high)
    def _():
        def body(c):
            early_copy(0, c).wait_recv()
            early_copy(1, c).wait_recv()

        each(0, early, body)

    blocks(lift_block(2), 0, 0, early * per)

    def second_rhs(c, acc):
        @pl.when(jnp.logical_and(has_high, c >= early))
        def _():
            lw_copy(c).wait_recv()

        acc = blocks(rhs_block(1), acc, c * per, (c + 1) * per)

        @pl.when(has_high)
        def _():
            z_copy(Z0, True, c).start()

        return acc

    div_sum, wet_sum, gamma = chunk_loop(second_rhs, acc)

    def around(Z, p, r):
        zb = Z[p, pl.ds(r, R + 2 * PAD), :]
        z = zb[PAD : PAD + R]
        n = R + 2 * PAD
        beside = pltpu.roll(zb, 1, 0)[PAD : PAD + R] + pltpu.roll(zb, n - 1, 0)[PAD : PAD + R]
        return z, beside + (to_right(z) + to_left(z))

    def image_block(r, delta):
        rs, rp = pl.ds(r, R), pl.ds(pl.multiple_of(r + PAD, 8), R)
        a, a_in = around(Z0, 1, r)
        b, b_in = around(Z0, 2, r)
        under = Z0[0, rp, :]
        image_a = H[0, rs, :] * a - (a_in + b + under)
        image_b = H[1, rs, :] * b - (b_in + a)
        Z1[1, rp, :] = G[0, rs, :] * image_a
        Z1[2, rp, :] = image_b
        return delta + fold(a * (image_a - under) + b * image_b)

    def first_image(c, delta):
        @pl.when(has_low)
        def _():
            z_copy(Z0, True, c).wait_recv()

        delta = blocks(image_block, delta, c * per, (c + 1) * per)

        @pl.when(has_low)
        def _():
            z_copy(Z1, False, c).start()

        return delta

    delta = chunk_loop(first_image, nil)
    red_send(1, 0, jnp.concatenate([lanes(x) for x in (div_sum, wet_sum, gamma, delta)], 0))

    def second_image(first, last):
        def body(c, x):
            @pl.when(has_high)
            def _():
                z_copy(Z0, False, c).wait_recv()

            def block(r, x):
                rs, rp = pl.ds(r, R), pl.ds(pl.multiple_of(r + PAD, 8), R)
                Z1[2, rp, :] = G[1, rs, :] * (Z1[2, rp, :] - Z0[3, rp, :])
                return x

            blocks(block, 0, c * per, (c + 1) * per)

            @pl.when(has_high)
            def _():
                z_copy(Z1, True, c).start()

            return x

        lax.fori_loop(first, last, body, 0)

    quarter = chunks // 4
    second_image(0, quarter)
    part = red_wait(1, 0, 32, jnp.add)
    red_send(1, 1, part)
    second_image(quarter, 2 * quarter)
    part = red_wait(1, 1, 32, jnp.add)
    red_send(1, 2, part)
    second_image(2 * quarter, 3 * quarter)
    part = red_wait(1, 2, 32, jnp.add)
    second_image(3 * quarter, chunks)
    div_squares = full(jnp.sum(part[0:8]))
    fluid_total = jnp.maximum(full(jnp.sum(part[8:16])), 1.0)
    gamma_0 = full(jnp.sum(part[16:24]))
    delta_0 = full(jnp.sum(part[24:32]))
    alpha_v = gamma_0 / delta_0
    alpha = alpha_v[0, 0]

    A2 = U

    def inner_block(r, acc):
        gamma, delta = acc
        rs, rp = pl.ds(r, R), pl.ds(pl.multiple_of(r + PAD, 8), R)
        a, a_in = around(Z1, 1, r)
        b, b_in = around(Z1, 2, r)
        under = Z1[0, rp, :]
        h_a, h_b = H[0, rs, :], H[1, rs, :]
        image_a = jnp.where(G[0, rs, :] > 0.0, h_a * a - (a_in + b + under), 0.0)
        image_b = jnp.where(G[1, rs, :] > 0.0, h_b * b - (b_in + a), 0.0)
        A2[0, rs, :] = image_a
        A2[1, rs, :] = image_b
        s_a, s_b = jnp.maximum(h_a, 1.0), jnp.maximum(h_b, 1.0)
        y_a = Z0[1, rp, :] - alpha * a
        y_b = Z0[2, rp, :] - alpha * b
        y_under = Z0[0, rp, :] - alpha * under
        gamma = gamma + fold(s_a * (y_a * y_a) + s_b * (y_b * y_b))
        t_a = (s_a * a - alpha * image_a) - y_under
        t_b = (s_b * b - alpha * image_b) + Z0[3, rp, :]
        delta = delta + fold(y_a * t_a + y_b * t_b)
        return gamma, delta

    def inner(c, acc):
        @pl.when(has_low)
        def _():
            z_copy(Z1, True, c).wait_recv()

        return blocks(inner_block, acc, c * per, (c + 1) * per)

    gamma, delta = chunk_loop(inner, (nil, nil))
    red_send(2, 0, jnp.concatenate([lanes(gamma), lanes(delta)], 0))
    part = red_wait(2, 0, 16, jnp.add)
    red_send(2, 1, part)
    part = red_wait(2, 1, 16, jnp.add)
    red_send(2, 2, part)
    part = red_wait(2, 2, 16, jnp.add)
    gamma_1 = full(jnp.sum(part[0:8]))
    delta_1 = full(jnp.sum(part[8:16]))
    beta = gamma_1 / gamma_0
    alpha_1 = gamma_1 / (delta_1 - beta * gamma_1 / alpha_v)
    c0_v = alpha_v + alpha_1 * (1.0 + beta)
    c1_v = -(alpha_v * alpha_1)
    scale_v = step_v / jnp.sqrt(div_squares / fluid_total + EPS)
    c0, c1, scale = c0_v[0, 0], c1_v[0, 0], scale_v[0, 0]

    def out_block(p, with_above):
        def body(r, x):
            rs, rp = pl.ds(r, R), pl.ds(pl.multiple_of(r + PAD, 8), R)
            z0, z1 = Z0[p + 1, rp, :], Z1[p + 1, rp, :]
            imp[p, rs, :] = time_step * (c0 * z0 + c1 * z1)
            second = A2[p, rs, :]
            if with_above:
                second = second - jnp.where(G[p, rs, :] > 0.0, Z1[3, rp, :], 0.0)
            rel[p, rs, :] = scale * (jnp.maximum(H[p, rs, :], 1.0) * (z0 - c0 * z1) - c1 * second)
            return x

        return body

    blocks(out_block(0, False), 0)

    def last(c, x):
        @pl.when(has_high)
        def _():
            z_copy(Z1, False, c).wait_recv()

        blocks(out_block(1, True), 0, c * per, (c + 1) * per)
        return x

    chunk_loop(last, 0)

    @pl.when(has_low)
    def _():
        flags_copy(False).wait_send()

        def sent_early(c):
            early_copy(0, c).wait_send()
            early_copy(1, c).wait_send()

        each(0, early, sent_early)
        each(early, chunks, lambda c: lw_copy(c).wait_send())

        def sent(c):
            z_copy(Z0, False, c).wait_send()
            z_copy(Z1, False, c).wait_send()

        each(0, chunks, sent)

    @pl.when(has_high)
    def _():
        flags_copy(True).wait_send()

        def sent(c):
            z_copy(Z0, True, c).wait_send()
            z_copy(Z1, True, c).wait_send()

        each(0, chunks, sent)

    red_end(0, 8)
    red_end(1, 32)
    red_end(2, 16)


def local(devices, u_face, v_face, w_face, smoke, obstacles):
    planes, rows, cols = u_face.shape
    chunks, early, loads = rows // CH, rows // CH // 4, rows // LOAD
    f32 = jnp.float32
    dma = pltpu.SemaphoreType.DMA
    out = jax.ShapeDtypeStruct((planes, rows, cols), f32)
    hbm = pl.BlockSpec(memory_space=pl.ANY)
    return pl.pallas_call(
        functools.partial(kernel, planes, rows, cols, devices),
        out_shape=(out, out),
        in_specs=[hbm] * 5,
        out_specs=(pl.BlockSpec(memory_space=pltpu.VMEM),) * 2,
        scratch_shapes=[
            pltpu.VMEM((planes, rows, cols), f32),
            pltpu.VMEM((planes, rows + PAD, cols), f32),
            pltpu.VMEM((planes + 1, rows, cols), f32),
            pltpu.VMEM((planes + 1, rows, cols), f32),
            pltpu.VMEM((planes + 2, rows // 32, cols), jnp.int32),
            pltpu.VMEM((3, planes, rows // 32, cols), jnp.int32),
            pltpu.VMEM((planes + 2, rows + 2 * PAD, cols), f32),
            pltpu.VMEM((planes + 2, rows + 2 * PAD, cols), f32),
            pltpu.VMEM((planes, rows, cols), f32),
            pltpu.VMEM((planes, rows, cols), f32),
            pltpu.VMEM((3, SLOTS, 32, 128), f32),
            pltpu.VMEM((8, 128), f32),
            dma((4, planes, loads)),
            dma,
            dma((2,)), dma((2,)),
            dma((2, early)), dma((2, early)),
            dma((chunks,)), dma((chunks,)),
            dma((chunks,)), dma((chunks,)),
            dma((chunks,)), dma((chunks,)),
            dma((chunks,)), dma((chunks,)),
            dma((chunks,)), dma((chunks,)),
            dma((3, SLOTS)), dma((3, SLOTS)),
        ],
        compiler_params=pltpu.CompilerParams(
            collective_id=0, has_side_effects=True, vmem_limit_bytes=67043328
        ),
        name="step",
    )(u_face, v_face, w_face, smoke, obstacles)


def solution(mesh):
    spec = P("gz", None, None)
    return jax.shard_map(
        functools.partial(local, mesh.shape["gz"]),
        mesh=mesh,
        in_specs=(spec,) * 5,
        out_specs=(spec, spec),
        check_vma=False,
    )
```
